128 devices in a mesh: area: 32 (over z_hi, x, y), inarea: 4 (over z_lo, core).
Axes of the slice: x: 4, y: 4, z: 4 (z_hi: 2, z_lo: 2; z = z_hi * 2 + z_lo), core: 2. Of those that a mesh axis runs over, the one named last changes fastest.
Arguments:
- spikes: int32 [2, 8, 65536], P(None, None, ('area', 'inarea')), may hold values 0 or 1
- release: float32 [8, 65536], P(None, ('area', 'inarea')), may hold values from 0.2 to 1
- potential: float32 [8, 65536], P(None, ('area', 'inarea')), may hold values from -6 to 6
- pre_trace: float32 [8, 65536], P(None, ('area', 'inarea')), may hold values from 0 to 2
- post_trace: float32 [8, 65536], P(None, ('area', 'inarea')), may hold values from 0 to 2
- w_local: float32 [65536, 2048], P(('area', 'inarea')), may hold values from -0.125 to 0.125
- w_long: float32 [65536, 3072], P(('area', 'inarea')), may hold values from -0.109375 to 0.109375
- sources: int32 [32, 12], replicated, may hold values from 0 to 255, as said below
- counts: int32 [32], replicated, may hold values from 512 to 2048, as said below
Outputs:
- voltage: float32 [8, 65536], P(None, ('area', 'inarea'))
- volley: float32 [8, 65536], P(None, ('area', 'inarea'))
- presyn: float32 [8, 65536], P(None, ('area', 'inarea'))
- postsyn: float32 [8, 65536], P(None, ('area', 'inarea'))
- local_new: float32 [65536, 2048], P(('area', 'inarea'))
- long_new: float32 [65536, 3072], P(('area', 'inarea'))
The draws below stay inside these ranges and needn't reach their ends.
Inputs may be any that keep to these rules, and one draw needn't show every extreme that they name: `sources`: no area takes a block of its own; the 12 blocks of one area lie in 12 different runs of 2 blocks that start at multiples of 2. `counts`: some area is full in every draw.
All inputs are finite; a program needn't handle non-finite values. No bound on the sum of `spikes` on one device may be relied on, other than what follows from the above.
Results may differ from the reference program's by a relative error of at most 0.0001.
Values sent between devices are 32-bit elements; how exact they have to be, the bound alone decides.
A program may use at most 128 MiB of HBM per device.

```python
import jax
import jax.numpy as jnp
from jax import lax

BLOCK = 256
NB_DEV = 2
SLOTS = 12
STEPS = 2
REPEAT_RUNS = 8
CORTICAL_PATCHES = 32
CELLS_PER_PATCH = 2048
NEURONS = 65536


def draw_sources(key, part):
    inner_size = CELLS_PER_PATCH // (NB_DEV * BLOCK)
    others = (CORTICAL_PATCHES - 1) * inner_size
    keys = jax.random.split(jax.random.fold_in(key, 11), CORTICAL_PATCHES)

    def one_area(area_key, area_index):
        order = jax.random.permutation(area_key, others)[:SLOTS].astype(jnp.int32)
        device = order + inner_size * (order >= area_index * inner_size).astype(jnp.int32)
        within = jax.random.randint(jax.random.fold_in(area_key, 7), (SLOTS,), 0, NB_DEV)
        return (device * NB_DEV + within).astype(jnp.int32)
    return jax.vmap(one_area)(keys, jnp.arange(CORTICAL_PATCHES, dtype=jnp.int32))


def draw_counts(key, part):
    base = jax.random.randint(jax.random.fold_in(key, 5), (CORTICAL_PATCHES,), CELLS_PER_PATCH // 4, CELLS_PER_PATCH + 1)
    filled = jax.random.randint(jax.random.fold_in(key, 3), (), 0, CORTICAL_PATCHES)
    return jnp.where(jnp.arange(CORTICAL_PATCHES) == filled, CELLS_PER_PATCH, base).astype(jnp.int32)


def set_ends(array, rng, least, top_value):
    longest = array.shape.index(max(array.shape))
    spots = []
    for shift in (0, 1):
        where = [jax.random.randint(jax.random.fold_in(rng, axis), (), 0, length) for axis, length in enumerate(array.shape)]
        where[longest] = (where[longest] + shift) % array.shape[longest]
        spots.append(tuple(where))
    return array.at[spots[0]].set(least).at[spots[1]].set(top_value)


def shard_levels(rng, extent, cuts, least, high):
    def one(position, blocks):
        steps = jax.random.uniform(jax.random.fold_in(jax.random.fold_in(rng, 6), position), (blocks,), jnp.float32, least / len(cuts), high / len(cuts))
        return jnp.repeat(jnp.exp(steps), extent[position] // blocks).reshape((-1,) + (1,) * (len(extent) - position - 1))

    level = one(*cuts[0])
    for cut in cuts[1:]:
        level = level * one(*cut)
    return level


def gaussian(stream_key, shape, width, bound, cuts=(), kind=jnp.bfloat16):
    drawn = width * jax.random.normal(stream_key, shape, jnp.float32)
    if cuts:
        drawn = drawn * shard_levels(stream_key, shape, cuts, -0.22, 0.18)
    return jnp.clip(drawn, -bound, bound).astype(kind)


def setup_inputs(seed: int = 0) -> dict:
    arg_keys = jax.random.split(jax.random.key(seed), 10)
    return {
        "spikes": set_ends((jax.random.randint(arg_keys[0], (STEPS, REPEAT_RUNS, NEURONS), 0, 2) < 1).astype(jnp.int32), jax.random.fold_in(arg_keys[0], 1), 0, 1),
        "release": jnp.clip(0.2 + 0.8 * jax.random.uniform(arg_keys[1], (REPEAT_RUNS, NEURONS), jnp.float32) ** shard_levels(arg_keys[1], (REPEAT_RUNS, NEURONS), ((1, 128),), -0.2, 0.2), 0.2, 1.0),
        "potential": gaussian(arg_keys[2], (REPEAT_RUNS, NEURONS), 1.0, 6.0, ((1, 128),), jnp.float32),
        "pre_trace": jnp.clip(2.0 * jax.random.uniform(arg_keys[3], (REPEAT_RUNS, NEURONS), jnp.float32) ** shard_levels(arg_keys[3], (REPEAT_RUNS, NEURONS), ((1, 128),), -0.2, 0.2), 0.0, 2.0),
        "post_trace": jnp.clip(2.0 * jax.random.uniform(arg_keys[4], (REPEAT_RUNS, NEURONS), jnp.float32) ** shard_levels(arg_keys[4], (REPEAT_RUNS, NEURONS), ((1, 128),), -0.2, 0.2), 0.0, 2.0),
        "w_local": gaussian(arg_keys[5], (NEURONS, CELLS_PER_PATCH), CELLS_PER_PATCH ** -0.5, 0.125, ((0, 128),), jnp.float32),
        "w_long": gaussian(arg_keys[6], (NEURONS, SLOTS * BLOCK), (SLOTS * BLOCK) ** -0.5, 0.109375, ((0, 128),), jnp.float32),
        "sources": draw_sources(jax.random.fold_in(arg_keys[9], 71), 0),
        "counts": draw_counts(jax.random.fold_in(arg_keys[9], 71), 0),
    }


ceiling_strength = lax.Precision.HIGHEST
pre_decay = 0.8
postsyn_trace_decay = 0.7
leak_factor = 0.9
adaptation_speed = 0.0005
recovery = 0.2
depletion = 0.5


def reference(spikes, release, potential, pre_trace, post_trace, w_local, w_long, sources, counts):
    positions = jnp.arange(CELLS_PER_PATCH, dtype=jnp.int32)
    active_flags = (positions[None, :] < counts[:, None]).reshape(NEURONS).astype(jnp.float32)
    nearby_coupling = w_local.reshape(CORTICAL_PATCHES, CELLS_PER_PATCH, CELLS_PER_PATCH)
    longrange_coupling = w_long.reshape(CORTICAL_PATCHES, CELLS_PER_PATCH, SLOTS * BLOCK)
    volley, presyn, postsyn, voltage = release, pre_trace, post_trace, potential
    for time_step_index in range(STEPS):
        emitted_pulses = spikes[time_step_index].astype(jnp.float32) * active_flags
        spike_activity = emitted_pulses * volley
        presyn = (pre_decay * presyn + spike_activity) * active_flags
        patch_cell_states = spike_activity.reshape(REPEAT_RUNS, CORTICAL_PATCHES, CELLS_PER_PATCH)
        sending_patch_side = presyn.reshape(REPEAT_RUNS, CORTICAL_PATCHES, CELLS_PER_PATCH)
        distal_cell_states = spike_activity.reshape(REPEAT_RUNS, NEURONS // BLOCK, BLOCK)[:, sources].reshape(REPEAT_RUNS, CORTICAL_PATCHES, SLOTS * BLOCK)
        distal_upstream_mark = presyn.reshape(REPEAT_RUNS, NEURONS // BLOCK, BLOCK)[:, sources].reshape(REPEAT_RUNS, CORTICAL_PATCHES, SLOTS * BLOCK)
        emitting_patch = emitted_pulses.reshape(REPEAT_RUNS, CORTICAL_PATCHES, CELLS_PER_PATCH)
        receiving_patch = postsyn.reshape(REPEAT_RUNS, CORTICAL_PATCHES, CELLS_PER_PATCH)
        current = jnp.einsum("tan,amn->tam", patch_cell_states, nearby_coupling, precision=ceiling_strength)
        current = current + jnp.einsum("tan,amn->tam", distal_cell_states, longrange_coupling, precision=ceiling_strength)
        voltage = (leak_factor * voltage + current.reshape(REPEAT_RUNS, NEURONS)) * active_flags
        nearby_coupling = nearby_coupling + adaptation_speed * (jnp.einsum("whk,whf->hkf", emitting_patch, sending_patch_side, precision=ceiling_strength) - jnp.einsum("whk,whf->hkf", receiving_patch, patch_cell_states, precision=ceiling_strength))
        longrange_coupling = longrange_coupling + adaptation_speed * (jnp.einsum("whk,whf->hkf", emitting_patch, distal_upstream_mark, precision=ceiling_strength) - jnp.einsum("whk,whf->hkf", receiving_patch, distal_cell_states, precision=ceiling_strength))
        postsyn = (postsyn_trace_decay * postsyn + emitted_pulses) * active_flags
        volley = volley + recovery * (1.0 - volley) - depletion * spike_activity
    return voltage, volley, presyn, postsyn, nearby_coupling.reshape(NEURONS, CELLS_PER_PATCH), longrange_coupling.reshape(NEURONS, SLOTS * BLOCK)
```

```python
import functools

import jax
import jax.numpy as jnp
from jax import lax
from jax.experimental import pallas as pl
from jax.experimental.pallas import tpu as pltpu
from jax.sharding import PartitionSpec as P

MESH = pl.DeviceIdType.MESH
BLOCK = 256
SLOTS = 12
TRIALS = 8
OWN = 512
AREA = 2048
FAR = SLOTS * BLOCK
ROWS = 128

pre_decay = 0.8
postsyn_trace_decay = 0.7
leak_factor = 0.9
adaptation_speed = 0.0005
recovery = 0.2
depletion = 0.5

AXES = (("x", "y", "z"), ("y", "z", "x"), ("z", "x", "y"))
OFFSETS = (1, 3, 2)


def device_of(place):
    area = lax.div(place["z"], 2) * 16 + place["x"] * 4 + place["y"]
    return (area, lax.rem(place["z"], 2) * 2 + place["c"])


def my_place():
    area, inner = lax.axis_index("area"), lax.axis_index("inarea")
    return {
        "x": lax.rem(lax.div(area, 4), 4),
        "y": lax.rem(area, 4),
        "z": lax.div(area, 16) * 2 + lax.div(inner, 2),
        "c": lax.rem(inner, 2),
    }


def moved(place, axis, offset):
    return {**place, axis: lax.rem(place[axis] + offset, 4)}


def remote(src, dst, send_sem, recv_sem, device):
    return pltpu.make_async_remote_copy(
        src_ref=src,
        dst_ref=dst,
        send_sem=send_sem,
        recv_sem=recv_sem,
        device_id=device,
        device_id_type=MESH,
    )


def early_dynamics(spikes, release, pre_trace, alive):
    firing_1 = spikes[0].astype(jnp.float32) * alive
    activity_1 = firing_1 * release
    presyn_1 = (pre_decay * pre_trace + activity_1) * alive
    volley_1 = release + recovery * (1.0 - release) - depletion * activity_1
    firing_2 = spikes[1].astype(jnp.float32) * alive
    activity_2 = firing_2 * volley_1
    return firing_1, activity_1, presyn_1, volley_1, firing_2, activity_2


def alive_of(counts_ref):
    area, inner = lax.axis_index("area"), lax.axis_index("inarea")
    position = inner * OWN + lax.broadcasted_iota(jnp.int32, (TRIALS, OWN), 1)
    return jnp.where(position < counts_ref[area], 1.0, 0.0).astype(jnp.float32)


def exchange_kernel(
    sources_ref, counts_ref, spikes_hbm, release_hbm, pre_hbm, w_local_hbm, w_long_hbm,
    near_ref, far_ref, w_local_ref, w_long_ref,
    spikes_ref, release_ref, pre_ref, gathered_0, gathered_1, gathered_2, staged, landed_0, landed_1, landed_2,
    load_sem, weight_sem, near_send, near_recv, send_1, recv_1, pair_send, pair_recv,
    send_2, recv_2, send_3, recv_3, send_4, recv_4,
):
    here = my_place()
    inner = lax.axis_index("inarea")
    core = here["c"]
    sibling = {**here, "c": 1 - core}
    gathered = (gathered_0, gathered_1, gathered_2)
    landed = (landed_0, landed_1, landed_2)

    loads = [
        pltpu.make_async_copy(spikes_hbm, spikes_ref, load_sem.at[0]),
        pltpu.make_async_copy(release_hbm, release_ref, load_sem.at[1]),
        pltpu.make_async_copy(pre_hbm, pre_ref, load_sem.at[2]),
    ]
    for load in loads:
        load.start()
    weights = [
        pltpu.make_async_copy(w_local_hbm, w_local_ref, weight_sem.at[0]),
        pltpu.make_async_copy(w_long_hbm, w_long_ref, weight_sem.at[1]),
    ]
    for load in weights:
        load.start()

    barrier = pltpu.get_barrier_semaphore()
    partners = [sibling]
    for axis in "xyz":
        for offset in (1, 2, 3):
            there = moved(here, axis, offset)
            partners += [there, {**there, "c": 1 - core}]
    for partner in partners:
        pl.semaphore_signal(barrier, inc=1, device_id=device_of(partner), device_id_type=MESH)

    for load in loads:
        load.wait()
    _, activity_1, presyn_1, _, _, activity_2 = early_dynamics(
        spikes_ref[...], release_ref[...], pre_ref[...], alive_of(counts_ref)
    )
    for kind, value in enumerate((activity_1, presyn_1, activity_2)):
        for half in range(2):
            for block in range(2):
                column = block * BLOCK + half * 128
                near_ref[inner, kind, half, block] = value[:, column : column + 128]
    for kind, (first, second, _) in enumerate(AXES):
        gathered[kind][here[second], here[first], core] = near_ref[inner, kind, core]
    pl.semaphore_wait(barrier, len(partners))

    steps_1 = []
    for kind, (first, second, _) in enumerate(AXES):
        target = gathered[kind].at[here[second], here[first], core]
        copies = [
            remote(
                near_ref.at[inner, kind, 1 - core], target, pair_send.at[kind], pair_recv.at[kind],
                device_of(sibling),
            )
        ]
        for j, offset in enumerate(OFFSETS):
            for other in range(2):
                half = core if other == 0 else 1 - core
                copies.append(
                    remote(
                        near_ref.at[inner, kind, half], target,
                        send_1.at[kind, j, other], recv_1.at[kind, j, other],
                        device_of({**moved(here, first, offset), "c": half}),
                    )
                )
        steps_1.append(copies)
    for copies in zip(*steps_1):
        for copy in copies:
            copy.start()
    near_copies = []
    for flip in range(1, 4):
        z = here["z"] if flip < 2 else here["z"] + 1 - 2 * lax.rem(here["z"], 2)
        c = core if flip == 2 else 1 - core
        near_copies.append(
            remote(
                near_ref.at[inner], near_ref.at[inner], near_send.at[flip - 1], near_recv.at[flip - 1],
                device_of({**here, "z": z, "c": c}),
            )
        )
    for copy in near_copies:
        copy.start()

    steps_2 = []
    for kind, (first, second, _) in enumerate(AXES):
        for copy in steps_1[kind]:
            copy.wait_recv()
        copies = [
            remote(
                gathered[kind].at[here[second]], gathered[kind].at[here[second]],
                send_2.at[kind, j], recv_2.at[kind, j], device_of(moved(here, second, offset)),
            )
            for j, offset in enumerate(OFFSETS)
        ]
        for copy in copies:
            copy.start()
        steps_2.append(copies)

    def source_place(area, slot):
        block = sources_ref[area, slot]
        run = lax.shift_right_logical(block, 1)
        return {
            "b": block & 1,
            "c": run & 1,
            "x": lax.shift_right_logical(run, 4) & 3,
            "y": lax.shift_right_logical(run, 2) & 3,
            "z": lax.shift_right_logical(run, 6) * 2 + (lax.shift_right_logical(run, 1) & 1),
        }

    def pick(kind, area, slot):
        source = source_place(area, slot)
        first, second, _ = AXES[kind]
        return gathered[kind][source[second], source[first], source["c"], source["b"]]

    steps_3 = []
    for kind, (_, _, third) in enumerate(AXES):
        for copy in steps_2[kind]:
            copy.wait_recv()
        copies = []
        for j, offset in enumerate(OFFSETS):
            there = moved(here, third, offset)
            area, _ = device_of(there)
            for slot in range(SLOTS):
                staged[kind, j, slot] = pick(kind, area, slot)
            copy = remote(
                staged.at[kind, j], landed[kind].at[here[third]],
                send_3.at[kind, j], recv_3.at[kind, j], device_of(there),
            )
            copy.start()
            copies.append(copy)
        steps_3.append(copies)
        for slot in range(SLOTS):
            landed[kind][here[third], slot] = pick(kind, lax.axis_index("area"), slot)

    steps_4 = []
    for kind, (_, _, third) in enumerate(AXES):
        for copy in steps_3[kind]:
            copy.wait_recv()
        for slot in range(SLOTS):
            plane = source_place(lax.axis_index("area"), slot)[third]
            far_ref[kind, core, slot] = landed[kind][plane, slot]
        copy = remote(
            far_ref.at[kind, core], far_ref.at[kind, core],
            send_4.at[kind], recv_4.at[kind], device_of(sibling),
        )
        copy.start()
        steps_4.append(copy)

    for copy in near_copies + steps_4:
        copy.wait_recv()
    for copies in steps_1 + steps_2 + steps_3 + [near_copies, steps_4]:
        for copy in copies:
            copy.wait_send()
    for load in weights:
        load.wait()


def split(value):
    high = value.astype(jnp.bfloat16)
    return high, (value - high.astype(jnp.float32)).astype(jnp.bfloat16)


def dot(a, b):
    return lax.dot_general(a, b, (((1,), (0,)), ((), ())), preferred_element_type=jnp.float32)


def synapse_kernel(
    counts_ref, near_ref, far_ref, w_local_ref, w_long_ref,
    spikes_ref, release_ref, potential_ref, pre_ref, post_ref,
    voltage_ref, volley_ref, presyn_ref, postsyn_ref, local_hbm, long_hbm,
    local_out, long_out, right_ref, act_ref, left_ref, current_ref, out_sem,
):
    alive = alive_of(counts_ref)
    firing_1, activity_1, presyn_1, volley_1, firing_2, activity_2 = early_dynamics(
        spikes_ref[...], release_ref[...], pre_ref[...], alive
    )
    post_1 = post_ref[...]
    post_2 = (postsyn_trace_decay * post_1 + firing_1) * alive
    presyn_ref[...] = (pre_decay * presyn_1 + activity_2) * alive
    postsyn_ref[...] = (postsyn_trace_decay * post_2 + firing_2) * alive
    volley_ref[...] = volley_1 + recovery * (1.0 - volley_1) - depletion * activity_2

    def high(value):
        return value.astype(jnp.bfloat16).astype(jnp.float32)

    minus_1, minus_2 = -post_1, -post_2
    left = jnp.concatenate(
        [
            firing_1, firing_1, firing_2, firing_2,
            high(minus_1), high(minus_1), minus_1 - high(minus_1),
            high(minus_2), high(minus_2), minus_2 - high(minus_2),
        ],
        axis=0,
    )
    left_ref[...] = left.T.astype(jnp.bfloat16)

    def sent(kind):
        near = [near_ref[i, kind, h, b] for i in range(4) for b in range(2) for h in range(2)]
        far = [far_ref[kind, h, s] for s in range(SLOTS) for h in range(2)]
        return jnp.concatenate(near + far, axis=1)

    act_1, pre_1, act_2 = sent(0), sent(1), sent(2)
    pre_2 = pre_decay * pre_1 + act_2
    parts = []
    for value in (pre_1, pre_2):
        big = high(adaptation_speed * value)
        parts += [big, adaptation_speed * value - big]
    for value in (act_1, act_2):
        big = high(adaptation_speed * value)
        parts += [big, adaptation_speed * value - big, big]
    right_ref[...] = jnp.concatenate(parts, axis=0).astype(jnp.bfloat16)

    both = jnp.concatenate([act_1, act_2], axis=0)
    big = high(both)
    act_ref[...] = jnp.concatenate([big, both - big], axis=0).T.astype(jnp.bfloat16)
    cross_high, cross_low = split(jnp.concatenate([pre_1, act_1], axis=0))
    cross = dot(cross_high, act_ref[...]) + dot(cross_low, act_ref[...])
    cross = adaptation_speed * (cross[:, 8:16] + cross[:, 24:32])

    def out_copies(step):
        rows = pl.ds(pl.multiple_of(step * ROWS, ROWS), ROWS)
        return (
            pltpu.make_async_copy(local_out.at[rows], local_hbm.at[rows], out_sem.at[0, step]),
            pltpu.make_async_copy(long_out.at[rows], long_hbm.at[rows], out_sem.at[1, step]),
        )

    @pl.loop(0, OWN // ROWS)
    def _(step):
        rows = pl.ds(pl.multiple_of(step * ROWS, ROWS), ROWS)
        w_near, w_far = w_local_ref[rows, :], w_long_ref[rows, :]
        near_high, near_low = split(w_near)
        far_high, far_low = split(w_far)
        current_ref[rows, :] = (
            dot(near_high, act_ref[:AREA, :]) + dot(near_low, act_ref[:AREA, :])
            + dot(far_high, act_ref[AREA:, :]) + dot(far_low, act_ref[AREA:, :])
        )
        local_out[rows, :] = w_near + dot(left_ref[rows, :], right_ref[:, :AREA])
        long_out[rows, :] = w_far + dot(left_ref[rows, :], right_ref[:, AREA:])
        for copy in out_copies(step):
            copy.start()

    current = current_ref[...].T
    current_1 = current[0:8] + current[16:24]
    current_2 = current[8:16] + current[24:32]
    extra = lax.dot_general(
        cross, jnp.concatenate([firing_1, -post_1], axis=0), (((0,), (0,)), ((), ())),
        preferred_element_type=jnp.float32, precision=lax.Precision.HIGHEST,
    )
    voltage_1 = (leak_factor * potential_ref[...] + current_1) * alive
    voltage_ref[...] = (leak_factor * voltage_1 + (current_2 + extra)) * alive

    @pl.loop(0, OWN // ROWS)
    def _(step):
        for copy in out_copies(step):
            copy.wait()


def local(spikes, release, potential, pre_trace, post_trace, w_local, w_long, sources, counts):
    smem = pl.BlockSpec(memory_space=pltpu.SMEM)
    hbm = pl.BlockSpec(memory_space=pltpu.HBM)
    vmem = pl.BlockSpec(memory_space=pltpu.VMEM)
    dma = pltpu.SemaphoreType.DMA
    f32 = jnp.float32
    in_hbm = functools.partial(pltpu.with_memory_space_constraint, memory_space=pltpu.HBM)
    near, far, w_local_in, w_long_in = pl.pallas_call(
        exchange_kernel,
        name="exchange",
        out_shape=(
            pltpu.VMEM((4, 3, 2, 2, TRIALS, 128), f32),
            pltpu.VMEM((3, 2, SLOTS, TRIALS, 128), f32),
            pltpu.VMEM((OWN, AREA), f32),
            pltpu.VMEM((OWN, FAR), f32),
        ),
        in_specs=[smem, smem, hbm, hbm, hbm, hbm, hbm],
        out_specs=(vmem, vmem, vmem, vmem),
        scratch_shapes=[
            pltpu.VMEM((2, TRIALS, OWN), jnp.int32),
            pltpu.VMEM((TRIALS, OWN), f32),
            pltpu.VMEM((TRIALS, OWN), f32),
            *[pltpu.VMEM((4, 4, 2, 2, TRIALS, 128), f32)] * 3,
            pltpu.VMEM((3, 3, SLOTS, TRIALS, 128), f32),
            *[pltpu.VMEM((4, SLOTS, TRIALS, 128), f32)] * 3,
            dma((3,)), dma((2,)), dma((3,)), dma((3,)),
            dma((3, 3, 2)), dma((3, 3, 2)), dma((3,)), dma((3,)),
            dma((3, 3)), dma((3, 3)), dma((3, 3)), dma((3, 3)), dma((3,)), dma((3,)),
        ],
        compiler_params=pltpu.CompilerParams(
            collective_id=0, has_side_effects=True, vmem_limit_bytes=20 << 20
        ),
    )(sources, counts, *(in_hbm(x) for x in (spikes, release, pre_trace, w_local, w_long)))

    columns = AREA + FAR
    return pl.pallas_call(
        synapse_kernel,
        name="synapses",
        out_shape=(
            *(jax.ShapeDtypeStruct((TRIALS, OWN), f32) for _ in range(4)),
            jax.ShapeDtypeStruct((OWN, AREA), f32),
            jax.ShapeDtypeStruct((OWN, FAR), f32),
        ),
        in_specs=[smem] + [vmem] * 9,
        out_specs=(vmem, vmem, vmem, vmem, hbm, hbm),
        scratch_shapes=[
            pltpu.VMEM((OWN, AREA), f32),
            pltpu.VMEM((OWN, FAR), f32),
            pltpu.VMEM((80, columns), jnp.bfloat16),
            pltpu.VMEM((columns, 32), jnp.bfloat16),
            pltpu.VMEM((OWN, 80), jnp.bfloat16),
            pltpu.VMEM((OWN, 32), f32),
            dma((2, OWN // ROWS)),
        ],
        compiler_params=pltpu.CompilerParams(vmem_limit_bytes=40 << 20),
    )(counts, near, far, w_local_in, w_long_in, spikes, release, potential, pre_trace, post_trace)


def solution(mesh):
    neurons = P(None, ("area", "inarea"))
    synapses = P(("area", "inarea"), None)
    return jax.shard_map(
        local,
        mesh=mesh,
        in_specs=(
            P(None, None, ("area", "inarea")), neurons, neurons, neurons, neurons,
            synapses, synapses, P(), P(),
        ),
        out_specs=(neurons, neurons, neurons, neurons, synapses, synapses),
        check_vma=False,
    )
```

```python
import functools

import jax
import jax.numpy as jnp
from jax import lax
from jax.experimental import pallas as pl
from jax.experimental.pallas import tpu as pltpu
from jax.sharding import PartitionSpec as P

MESH = pl.DeviceIdType.MESH
BLOCK = 256
SLOTS = 12
TRIALS = 8
OWN = 512
AREA = 2048
FAR = SLOTS * BLOCK
ROWS = 128
TILE = (TRIALS, 128)

pre_decay = 0.8
postsyn_trace_decay = 0.7
leak_factor = 0.9
adaptation_speed = 0.0005
recovery = 0.2
depletion = 0.5

AXES = (("x", "y", "z"), ("y", "z", "x"), ("z", "x", "y"))
OFFSETS = (1, 3, 2)


def device_of(place):
    area = lax.div(place["z"], 2) * 16 + place["x"] * 4 + place["y"]
    return (area, lax.rem(place["z"], 2) * 2 + place["c"])


def my_place():
    area, inner = lax.axis_index("area"), lax.axis_index("inarea")
    return {
        "x": lax.rem(lax.div(area, 4), 4),
        "y": lax.rem(area, 4),
        "z": lax.div(area, 16) * 2 + lax.div(inner, 2),
        "c": lax.rem(inner, 2),
    }


def moved(place, axis, offset):
    return {**place, axis: lax.rem(place[axis] + offset, 4)}


def remote(src, dst, send_sem, recv_sem, device):
    return pltpu.make_async_remote_copy(
        src_ref=src,
        dst_ref=dst,
        send_sem=send_sem,
        recv_sem=recv_sem,
        device_id=device,
        device_id_type=MESH,
    )


def early_dynamics(spikes, release, pre_trace, alive):
    firing_1 = spikes[0].astype(jnp.float32) * alive
    activity_1 = firing_1 * release
    presyn_1 = (pre_decay * pre_trace + activity_1) * alive
    volley_1 = release + recovery * (1.0 - release) - depletion * activity_1
    firing_2 = spikes[1].astype(jnp.float32) * alive
    activity_2 = firing_2 * volley_1
    return firing_1, activity_1, presyn_1, volley_1, firing_2, activity_2


def alive_of(counts_ref):
    area, inner = lax.axis_index("area"), lax.axis_index("inarea")
    position = inner * OWN + lax.broadcasted_iota(jnp.int32, (TRIALS, OWN), 1)
    return jnp.where(position < counts_ref[area], 1.0, 0.0).astype(jnp.float32)


def high(value):
    return value.astype(jnp.bfloat16).astype(jnp.float32)


def halves(value):
    big = high(value)
    return big, value - big


def dot(a, b):
    return lax.dot_general(a, b, (((1,), (0,)), ((), ())), preferred_element_type=jnp.float32)


def dot_t(a, b):
    return lax.dot_general(a, b, (((1,), (1,)), ((), ())), preferred_element_type=jnp.float32)


def left_matrix(firing_1, firing_2, post_1, post_2):
    big_1, small_1 = halves(-post_1)
    big_2, small_2 = halves(-post_2)
    parts = [firing_1, firing_1, firing_2, firing_2, big_1, big_1, small_1, big_2, big_2, small_2]
    return jnp.concatenate(parts, axis=0).T.astype(jnp.bfloat16)


def right_matrix(act_1, pre_1, act_2):
    parts = []
    for value in (pre_1, pre_decay * pre_1 + act_2):
        parts += halves(adaptation_speed * value)
    for value in (act_1, act_2):
        big, small = halves(adaptation_speed * value)
        parts += [big, small, big]
    return jnp.concatenate(parts, axis=0).astype(jnp.bfloat16)


def activity_matrix(act_1, act_2):
    return jnp.concatenate(halves(jnp.concatenate([act_1, act_2], axis=0)), axis=0).astype(jnp.bfloat16)


def cross_products(act_1, pre_1, activity):
    big, small = halves(jnp.concatenate([pre_1, act_1], axis=0))
    return dot_t(big.astype(jnp.bfloat16), activity) + dot_t(small.astype(jnp.bfloat16), activity)


def row_block(step, rows=ROWS):
    return pl.ds(pl.multiple_of(step * rows, rows), rows)


def exchange_kernel(
    sources_hbm, counts_hbm, spikes_hbm, release_hbm, pre_hbm, post_hbm, w_local_hbm, w_long_hbm,
    far_ref, local_ref, w_long_ref, high_ref, low_ref, left_ref, current_ref, cross_ref, alive_ref,
    sources_ref, counts_ref, index_ref,
    spikes_ref, release_ref, pre_ref, post_ref, near_ref, gathered_0, gathered_1, gathered_2, staged,
    landed_0, landed_1, landed_2, right_ref, activity_ref,
    load_sem, source_sem, weight_sem, near_recv, recv_1, recv_2, recv_3, recv_4, send_sem,
):
    here = my_place()
    inner = lax.axis_index("inarea")
    core = here["c"]
    sibling = {**here, "c": 1 - core}
    gathered = (gathered_0, gathered_1, gathered_2)
    landed = (landed_0, landed_1, landed_2)

    loads = [
        pltpu.make_async_copy(src, dst, load_sem.at[i])
        for i, (src, dst) in enumerate(
            (
                (counts_hbm, counts_ref), (spikes_hbm, spikes_ref), (release_hbm, release_ref),
                (pre_hbm, pre_ref), (post_hbm, post_ref),
            )
        )
    ]
    for load in loads:
        load.start()
    source_load = pltpu.make_async_copy(sources_hbm, sources_ref, source_sem)
    source_load.start()
    weight_loads = [
        pltpu.make_async_copy(w_long_hbm, w_long_ref, weight_sem.at[0]),
        pltpu.make_async_copy(w_local_hbm, local_ref, weight_sem.at[1]),
    ]
    for load in weight_loads:
        load.start()

    barrier = pltpu.get_barrier_semaphore()
    partners = [sibling]
    for axis in "xyz":
        for offset in (1, 2, 3):
            there = moved(here, axis, offset)
            partners += [there, {**there, "c": 1 - core}]
    for partner in partners:
        pl.semaphore_signal(barrier, inc=1, device_id=device_of(partner), device_id_type=MESH)

    for load in loads:
        load.wait()
    alive = alive_of(counts_ref)
    firing_1, activity_1, presyn_1, _, firing_2, activity_2 = early_dynamics(
        spikes_ref[...], release_ref[...], pre_ref[...], alive
    )
    for kind, value in enumerate((activity_1, presyn_1, activity_2)):
        for half in range(2):
            for block in range(2):
                column = block * BLOCK + half * 128
                near_ref[inner * 12 + kind * 4 + half * 2 + block] = value[:, column : column + 128]

    def mine(kind, half):
        return pl.ds(inner * 12 + kind * 4 + half * 2, 2)

    spots = [here[second] * 16 + here[first] * 4 + core * 2 for first, second, _ in AXES]
    for kind in range(3):
        gathered[kind][pl.ds(spots[kind], 2)] = near_ref[mine(kind, core)]
    pl.semaphore_wait(barrier, len(partners))

    def arrived(ref, sem):
        pltpu.make_async_copy(ref, ref, sem).wait()

    def step_1(kind, place, half):
        remote(
            near_ref.at[mine(kind, half)], gathered[kind].at[pl.ds(spots[kind], 2)],
            send_sem.at[0], recv_1.at[kind], device_of({**place, "c": half}),
        ).start()

    for offset in OFFSETS:
        for kind, (first, _, _) in enumerate(AXES):
            there = moved(here, first, offset)
            step_1(kind, there, core)
            step_1(kind, there, 1 - core)
    for kind in range(3):
        step_1(kind, here, 1 - core)
    for flip in range(1, 4):
        z = here["z"] if flip < 2 else here["z"] + 1 - 2 * lax.rem(here["z"], 2)
        c = core if flip == 2 else 1 - core
        remote(
            near_ref.at[pl.ds(inner * 12, 12)], near_ref.at[pl.ds(inner * 12, 12)],
            send_sem.at[1], near_recv, device_of({**here, "z": z, "c": c}),
        ).start()

    source_load.wait()

    def note_indices(slot, area):
        block = sources_ref[slot, area]
        run = lax.shift_right_logical(block, 1)
        return {
            "cb": (run & 1) * 2 + (block & 1),
            "x": lax.shift_right_logical(run, 4) & 3,
            "y": lax.shift_right_logical(run, 2) & 3,
            "z": lax.shift_right_logical(run, 6) * 2 + (lax.shift_right_logical(run, 1) & 1),
        }

    def spot_of(kind, source):
        first, second, _ = AXES[kind]
        return source[second] * 16 + source[first] * 4 + source["cb"]

    @pl.loop(0, SLOTS)
    def _(slot):
        own = note_indices(slot, lax.axis_index("area"))
        for kind, (_, _, third) in enumerate(AXES):
            index_ref[kind * 5 + 3, slot] = spot_of(kind, own)
            index_ref[kind * 5 + 4, slot] = own[third] * SLOTS + slot
            for j, offset in enumerate(OFFSETS):
                area, _ = device_of(moved(here, third, offset))
                index_ref[kind * 5 + j, slot] = spot_of(kind, note_indices(slot, area))

    alive_ref[...] = alive
    post_1 = post_ref[...]
    post_2 = (postsyn_trace_decay * post_1 + firing_1) * alive
    left_ref[...] = left_matrix(firing_1, firing_2, post_1, post_2)
    weight_loads[0].wait()

    @pl.loop(0, OWN // 32)
    def _(step):
        rows = row_block(step, 32)
        value = w_long_ref[rows, :]
        big = value.astype(jnp.bfloat16)
        high_ref[rows, :] = big
        low_ref[rows, :] = (value - big.astype(jnp.float32)).astype(jnp.bfloat16)

    for kind, (first, second, _) in enumerate(AXES):
        arrived(gathered[kind].at[pl.ds(0, 14)], recv_1.at[kind])
        part = gathered[kind].at[pl.ds(here[second] * 16, 16)]
        for offset in OFFSETS:
            remote(
                part, part, send_sem.at[2], recv_2.at[kind], device_of(moved(here, second, offset))
            ).start()

    arrived(near_ref.at[pl.ds(0, 36)], near_recv)
    act_1, pre_1, act_2 = (
        jnp.concatenate(
            [near_ref[i * 12 + kind * 4 + h * 2 + b] for i in range(4) for b in range(2) for h in range(2)],
            axis=1,
        )
        for kind in range(3)
    )
    right_ref[...] = right_matrix(act_1, pre_1, act_2)
    activity_ref[...] = activity_matrix(act_1, act_2)
    cross_ref[...] = cross_products(act_1, pre_1, activity_ref[...])
    weight_loads[1].wait()

    @pl.loop(0, OWN // ROWS)
    def _(step):
        rows = row_block(step)
        value = local_ref[rows, :]
        big = value.astype(jnp.bfloat16)
        small = (value - big.astype(jnp.float32)).astype(jnp.bfloat16)
        current_ref[rows, :] = dot_t(big, activity_ref[...]) + dot_t(small, activity_ref[...])
        local_ref[rows, :] = value + dot(left_ref[rows, :], right_ref[...])

    for kind, (_, _, third) in enumerate(AXES):
        arrived(gathered[kind].at[pl.ds(0, 48)], recv_2.at[kind])
        for j, offset in enumerate(OFFSETS):
            first = (kind * 3 + j) * SLOTS
            for slot in range(SLOTS):
                staged[first + slot] = gathered[kind][index_ref[kind * 5 + j, slot]]
            remote(
                staged.at[pl.ds(first, SLOTS)], landed[kind].at[pl.ds(here[third] * SLOTS, SLOTS)],
                send_sem.at[3], recv_3.at[kind], device_of(moved(here, third, offset)),
            ).start()
        for slot in range(SLOTS):
            landed[kind][here[third] * SLOTS + slot] = gathered[kind][index_ref[kind * 5 + 3, slot]]

    for kind in range(3):
        arrived(landed[kind].at[pl.ds(0, 36)], recv_3.at[kind])
        first = kind * 24 + core * SLOTS
        for slot in range(SLOTS):
            far_ref[first + slot] = landed[kind][index_ref[kind * 5 + 4, slot]]
        part = far_ref.at[pl.ds(first, SLOTS)]
        remote(part, part, send_sem.at[4], recv_4, device_of(sibling)).start()

    arrived(far_ref.at[pl.ds(0, 36)], recv_4)
    for i, ref in enumerate(
        (
            gathered_0.at[pl.ds(0, 42)], near_ref.at[pl.ds(0, 36)], w_long_ref.at[pl.ds(0, 48)],
            staged, far_ref.at[pl.ds(0, 36)],
        )
    ):
        arrived(ref, send_sem.at[i])


def synapse_kernel(
    far_ref, local_ref, w_long_ref, high_ref, low_ref, left_ref, current_near, cross_near, alive_ref,
    spikes_ref, release_ref, potential_ref, pre_ref, post_ref,
    voltage_ref, volley_ref, presyn_ref, postsyn_ref, local_hbm, long_hbm,
    long_out, right_ref, activity_ref, current_ref, out_sem,
):
    local_copy = pltpu.make_async_copy(local_ref, local_hbm, out_sem.at[OWN // ROWS])
    local_copy.start()
    act_1, pre_1, act_2 = (
        jnp.concatenate([far_ref[kind * 24 + h * SLOTS + s] for s in range(SLOTS) for h in range(2)], axis=1)
        for kind in range(3)
    )
    right_ref[...] = right_matrix(act_1, pre_1, act_2)
    activity_ref[...] = activity_matrix(act_1, act_2)

    def long_copy(step):
        rows = row_block(step)
        return pltpu.make_async_copy(long_out.at[rows], long_hbm.at[rows], out_sem.at[step])

    @pl.loop(0, OWN // ROWS)
    def _(step):
        rows = row_block(step)
        long_out[rows, :] = w_long_ref[rows, :] + dot(left_ref[rows, :], right_ref[...])
        long_copy(step).start()

    @pl.loop(0, OWN // ROWS)
    def _(step):
        rows = row_block(step)
        current_ref[rows, :] = (
            current_near[rows, :]
            + dot_t(high_ref[rows, :], activity_ref[...]) + dot_t(low_ref[rows, :], activity_ref[...])
        )

    alive = alive_ref[...]
    firing_1, activity_1, presyn_1, volley_1, firing_2, activity_2 = early_dynamics(
        spikes_ref[...], release_ref[...], pre_ref[...], alive
    )
    post_1 = post_ref[...]
    post_2 = (postsyn_trace_decay * post_1 + firing_1) * alive
    presyn_ref[...] = (pre_decay * presyn_1 + activity_2) * alive
    postsyn_ref[...] = (postsyn_trace_decay * post_2 + firing_2) * alive
    volley_ref[...] = volley_1 + recovery * (1.0 - volley_1) - depletion * activity_2

    cross = cross_near[...] + cross_products(act_1, pre_1, activity_ref[...])
    cross = adaptation_speed * (cross[:, 8:16] + cross[:, 24:32])
    current = current_ref[...].T
    current_1 = current[0:8] + current[16:24]
    current_2 = current[8:16] + current[24:32]
    extra = lax.dot_general(
        cross, jnp.concatenate([firing_1, -post_1], axis=0), (((0,), (0,)), ((), ())),
        preferred_element_type=jnp.float32, precision=lax.Precision.HIGHEST,
    )
    voltage_1 = (leak_factor * potential_ref[...] + current_1) * alive
    voltage_ref[...] = (leak_factor * voltage_1 + (current_2 + extra)) * alive

    @pl.loop(0, OWN // ROWS)
    def _(step):
        long_copy(step).wait()
    local_copy.wait()


def local(spikes, release, potential, pre_trace, post_trace, w_local, w_long, sources, counts):
    hbm = pl.BlockSpec(memory_space=pltpu.HBM)
    vmem = pl.BlockSpec(memory_space=pltpu.VMEM)
    dma = pltpu.SemaphoreType.DMA
    f32, bf16 = jnp.float32, jnp.bfloat16
    in_hbm = functools.partial(pltpu.with_memory_space_constraint, memory_space=pltpu.HBM)
    parts = pl.pallas_call(
        exchange_kernel,
        name="exchange",
        out_shape=(
            pltpu.VMEM((72, *TILE), f32),
            pltpu.VMEM((OWN, AREA), f32),
            pltpu.VMEM((OWN, FAR), f32),
            pltpu.VMEM((OWN, FAR), bf16),
            pltpu.VMEM((OWN, FAR), bf16),
            pltpu.VMEM((OWN, 80), bf16),
            pltpu.VMEM((OWN, 32), f32),
            pltpu.VMEM((16, 32), f32),
            pltpu.VMEM((TRIALS, OWN), f32),
        ),
        in_specs=[hbm] * 8,
        out_specs=(vmem,) * 9,
        scratch_shapes=[
            pltpu.SMEM((SLOTS, 32), jnp.int32),
            pltpu.SMEM((32,), jnp.int32),
            pltpu.SMEM((15, SLOTS), jnp.int32),
            pltpu.VMEM((2, TRIALS, OWN), jnp.int32),
            *[pltpu.VMEM((TRIALS, OWN), f32)] * 3,
            pltpu.VMEM((48, *TILE), f32),
            *[pltpu.VMEM((64, *TILE), f32)] * 3,
            pltpu.VMEM((108, *TILE), f32),
            *[pltpu.VMEM((48, *TILE), f32)] * 3,
            pltpu.VMEM((80, AREA), bf16),
            pltpu.VMEM((32, AREA), bf16),
            dma((5,)), dma, dma((2,)), dma, dma((3,)), dma((3,)), dma((3,)), dma, dma((5,)),
        ],
        compiler_params=pltpu.CompilerParams(
            collective_id=0, has_side_effects=True, vmem_limit_bytes=28 << 20
        ),
    )(
        in_hbm(sources.T), in_hbm(counts),
        *(in_hbm(x) for x in (spikes, release, pre_trace, post_trace, w_local, w_long)),
    )
    return pl.pallas_call(
        synapse_kernel,
        name="synapses",
        out_shape=(
            *(jax.ShapeDtypeStruct((TRIALS, OWN), f32) for _ in range(4)),
            jax.ShapeDtypeStruct((OWN, AREA), f32),
            jax.ShapeDtypeStruct((OWN, FAR), f32),
        ),
        in_specs=[vmem] * 14,
        out_specs=(vmem, vmem, vmem, vmem, hbm, hbm),
        scratch_shapes=[
            pltpu.VMEM((OWN, FAR), f32),
            pltpu.VMEM((80, FAR), bf16),
            pltpu.VMEM((32, FAR), bf16),
            pltpu.VMEM((OWN, 32), f32),
            dma((OWN // ROWS + 1,)),
        ],
        compiler_params=pltpu.CompilerParams(vmem_limit_bytes=34 << 20),
    )(*parts, spikes, release, potential, pre_trace, post_trace)


def solution(mesh):
    neurons = P(None, ("area", "inarea"))
    synapses = P(("area", "inarea"), None)
    return jax.shard_map(
        local,
        mesh=mesh,
        in_specs=(
            P(None, None, ("area", "inarea")), neurons, neurons, neurons, neurons,
            synapses, synapses, P(), P(),
        ),
        out_specs=(neurons, neurons, neurons, neurons, synapses, synapses),
        check_vma=False,
    )
```

```python
import functools

import jax
import jax.numpy as jnp
from jax import lax
from jax.experimental import pallas as pl
from jax.experimental.pallas import tpu as pltpu
from jax.sharding import PartitionSpec as P

MESH = pl.DeviceIdType.MESH
BLOCK = 256
SLOTS = 12
TRIALS = 8
OWN = 512
AREA = 2048
FAR = SLOTS * BLOCK
ROWS = 128
TILE = (TRIALS, 128)

pre_decay = 0.8
postsyn_trace_decay = 0.7
leak_factor = 0.9
adaptation_speed = 0.0005
recovery = 0.2
depletion = 0.5

AXES = (("x", "y", "z"), ("y", "z", "x"), ("z", "x", "y"))
OFFSETS = (2, 1, 3)


def device_of(place):
    area = lax.div(place["z"], 2) * 16 + place["x"] * 4 + place["y"]
    return (area, lax.rem(place["z"], 2) * 2 + place["c"])


def my_place():
    area, inner = lax.axis_index("area"), lax.axis_index("inarea")
    return {
        "x": lax.rem(lax.div(area, 4), 4),
        "y": lax.rem(area, 4),
        "z": lax.div(area, 16) * 2 + lax.div(inner, 2),
        "c": lax.rem(inner, 2),
    }


def moved(place, axis, offset):
    return {**place, axis: lax.rem(place[axis] + offset, 4)}


def remote(src, dst, send_sem, recv_sem, device):
    return pltpu.make_async_remote_copy(
        src_ref=src,
        dst_ref=dst,
        send_sem=send_sem,
        recv_sem=recv_sem,
        device_id=device,
        device_id_type=MESH,
    )


def early_dynamics(spikes, release, pre_trace, alive):
    firing_1 = spikes[0].astype(jnp.float32) * alive
    activity_1 = firing_1 * release
    presyn_1 = (pre_decay * pre_trace + activity_1) * alive
    volley_1 = release + recovery * (1.0 - release) - depletion * activity_1
    firing_2 = spikes[1].astype(jnp.float32) * alive
    activity_2 = firing_2 * volley_1
    return firing_1, activity_1, presyn_1, volley_1, firing_2, activity_2


def alive_of(counts_ref):
    area, inner = lax.axis_index("area"), lax.axis_index("inarea")
    position = inner * OWN + lax.broadcasted_iota(jnp.int32, (TRIALS, OWN), 1)
    return jnp.where(position < counts_ref[area], 1.0, 0.0).astype(jnp.float32)


def high(value):
    return value.astype(jnp.bfloat16).astype(jnp.float32)


def halves(value):
    big = high(value)
    return big, value - big


def dot(a, b):
    return lax.dot_general(a, b, (((1,), (0,)), ((), ())), preferred_element_type=jnp.float32)


def dot_t(a, b):
    return lax.dot_general(a, b, (((1,), (1,)), ((), ())), preferred_element_type=jnp.float32)


def left_matrix(firing_1, firing_2, post_1, post_2):
    big_1, small_1 = halves(-post_1)
    big_2, small_2 = halves(-post_2)
    parts = [firing_1, firing_1, firing_2, firing_2, big_1, big_1, small_1, big_2, big_2, small_2]
    return jnp.concatenate(parts, axis=0).T.astype(jnp.bfloat16)


def right_matrix(act_1, pre_1, act_2):
    parts = []
    for value in (pre_1, pre_decay * pre_1 + act_2):
        parts += halves(adaptation_speed * value)
    for value in (act_1, act_2):
        big, small = halves(adaptation_speed * value)
        parts += [big, small, big]
    return jnp.concatenate(parts, axis=0).astype(jnp.bfloat16)


def activity_matrix(act_1, act_2):
    return jnp.concatenate(halves(jnp.concatenate([act_1, act_2], axis=0)), axis=0).astype(jnp.bfloat16)


def cross_products(act_1, pre_1, activity):
    big, small = halves(jnp.concatenate([pre_1, act_1], axis=0))
    return dot_t(big.astype(jnp.bfloat16), activity) + dot_t(small.astype(jnp.bfloat16), activity)


def row_block(step, rows=ROWS):
    return pl.ds(pl.multiple_of(step * rows, rows), rows)


def exchange_kernel(
    sources_hbm, counts_hbm, spikes_hbm, release_hbm, pre_hbm, post_hbm, w_local_hbm, w_long_hbm,
    far_ref, local_ref, w_long_ref, high_ref, low_ref, left_ref, current_ref, cross_ref, alive_ref,
    sources_ref, counts_ref, index_ref,
    spikes_ref, release_ref, pre_ref, post_ref, near_ref, gathered_0, gathered_1, gathered_2, staged,
    landed_0, landed_1, landed_2, right_ref, activity_ref,
    load_sem, source_sem, weight_sem, near_recv, recv_1, recv_2, recv_3, recv_4, send_sem,
):
    here = my_place()
    inner = lax.axis_index("inarea")
    core = here["c"]
    sibling = {**here, "c": 1 - core}
    gathered = (gathered_0, gathered_1, gathered_2)
    landed = (landed_0, landed_1, landed_2)

    loads = [
        pltpu.make_async_copy(src, dst, load_sem.at[i])
        for i, (src, dst) in enumerate(
            (
                (counts_hbm, counts_ref), (spikes_hbm, spikes_ref), (release_hbm, release_ref),
                (pre_hbm, pre_ref), (post_hbm, post_ref),
            )
        )
    ]
    for load in loads:
        load.start()
    source_load = pltpu.make_async_copy(sources_hbm, sources_ref, source_sem)
    source_load.start()
    weight_loads = [
        pltpu.make_async_copy(w_long_hbm, w_long_ref, weight_sem.at[0]),
        pltpu.make_async_copy(w_local_hbm, local_ref, weight_sem.at[1]),
    ]
    for load in weight_loads:
        load.start()

    barrier = pltpu.get_barrier_semaphore()
    partners = [sibling]
    for axis in "xyz":
        for offset in (1, 2, 3):
            there = moved(here, axis, offset)
            partners += [there, {**there, "c": 1 - core}]
    for partner in partners:
        pl.semaphore_signal(barrier, inc=1, device_id=device_of(partner), device_id_type=MESH)

    for load in loads:
        load.wait()
    alive = alive_of(counts_ref)
    firing_1, activity_1, presyn_1, _, firing_2, activity_2 = early_dynamics(
        spikes_ref[...], release_ref[...], pre_ref[...], alive
    )
    for kind, value in enumerate((activity_1, presyn_1, activity_2)):
        for half in range(2):
            for block in range(2):
                column = block * BLOCK + half * 128
                near_ref[inner * 12 + kind * 4 + half * 2 + block] = value[:, column : column + 128]

    def mine(kind, half):
        return pl.ds(inner * 12 + kind * 4 + half * 2, 2)

    spots = [here[second] * 16 + here[first] * 4 + core * 2 for first, second, _ in AXES]
    for kind in range(3):
        gathered[kind][pl.ds(spots[kind], 2)] = near_ref[mine(kind, core)]
    pl.semaphore_wait(barrier, len(partners))

    def arrived(ref, sem):
        pltpu.make_async_copy(ref, ref, sem).wait()

    def step_1(kind, place, half, j):
        remote(
            near_ref.at[mine(kind, half)], gathered[kind].at[pl.ds(spots[kind], 2)],
            send_sem.at[0], recv_1.at[kind, j], device_of({**place, "c": half}),
        ).start()

    for kind in range(3):
        step_1(kind, here, 1 - core, 3)
    for j, offset in enumerate(OFFSETS):
        for kind, (first, _, _) in enumerate(AXES):
            there = moved(here, first, offset)
            step_1(kind, there, core, j)
            step_1(kind, there, 1 - core, j)
    across = {**here, "z": here["z"] + 1 - 2 * lax.rem(here["z"], 2)}
    across_inner = lax.rem(inner + 2, 4)

    def pass_near(owner, place, number):
        part = near_ref.at[pl.ds(owner * 12, 12)]
        remote(part, part, send_sem.at[1], near_recv.at[number], device_of(place)).start()

    pass_near(inner, sibling, 0)
    pass_near(inner, across, 1)

    source_load.wait()

    def note_indices(slot, area):
        block = sources_ref[slot, area]
        run = lax.shift_right_logical(block, 1)
        return {
            "cb": (run & 1) * 2 + (block & 1),
            "x": lax.shift_right_logical(run, 4) & 3,
            "y": lax.shift_right_logical(run, 2) & 3,
            "z": lax.shift_right_logical(run, 6) * 2 + (lax.shift_right_logical(run, 1) & 1),
        }

    def spot_of(kind, source):
        first, second, _ = AXES[kind]
        return source[second] * 16 + source[first] * 4 + source["cb"]

    @pl.loop(0, SLOTS)
    def _(slot):
        own = note_indices(slot, lax.axis_index("area"))
        for kind, (_, _, third) in enumerate(AXES):
            index_ref[kind * 5 + 3, slot] = spot_of(kind, own)
            index_ref[kind * 5 + 4, slot] = own[third] * SLOTS + slot
            for j, offset in enumerate(OFFSETS):
                area, _ = device_of(moved(here, third, offset))
                index_ref[kind * 5 + j, slot] = spot_of(kind, note_indices(slot, area))

    alive_ref[...] = alive
    post_1 = post_ref[...]
    post_2 = (postsyn_trace_decay * post_1 + firing_1) * alive
    left_ref[...] = left_matrix(firing_1, firing_2, post_1, post_2)

    def step_2(kind, j):
        first, second, _ = AXES[kind]
        origin = here[first] if j == 3 else lax.rem(here[first] + 4 - OFFSETS[j], 4)
        part = gathered[kind].at[pl.ds(here[second] * 16 + origin * 4, 4)]
        arrived(part if j < 3 else part.at[pl.ds(0, 2)], recv_1.at[kind, j])
        for offset in OFFSETS:
            remote(
                part, part, send_sem.at[2], recv_2.at[kind], device_of(moved(here, second, offset))
            ).start()

    for kind in range(3):
        step_2(kind, 3)
    weight_loads[0].wait()

    @pl.loop(0, OWN // 32)
    def _(step):
        rows = row_block(step, 32)
        value = w_long_ref[rows, :]
        big = value.astype(jnp.bfloat16)
        high_ref[rows, :] = big
        low_ref[rows, :] = (value - big.astype(jnp.float32)).astype(jnp.bfloat16)

    for j in (1, 2, 0):
        for kind in range(3):
            step_2(kind, j)

    arrived(near_ref.at[pl.ds(0, 12)], near_recv.at[1])
    pass_near(across_inner, sibling, 2)
    arrived(near_ref.at[pl.ds(0, 12)], near_recv.at[0])
    arrived(near_ref.at[pl.ds(0, 12)], near_recv.at[2])
    act_1, pre_1, act_2 = (
        jnp.concatenate(
            [near_ref[i * 12 + kind * 4 + h * 2 + b] for i in range(4) for b in range(2) for h in range(2)],
            axis=1,
        )
        for kind in range(3)
    )
    right_ref[...] = right_matrix(act_1, pre_1, act_2)
    activity_ref[...] = activity_matrix(act_1, act_2)
    cross_ref[...] = cross_products(act_1, pre_1, activity_ref[...])
    weight_loads[1].wait()

    @pl.loop(0, OWN // ROWS)
    def _(step):
        rows = row_block(step)
        value = local_ref[rows, :]
        big = value.astype(jnp.bfloat16)
        small = (value - big.astype(jnp.float32)).astype(jnp.bfloat16)
        current_ref[rows, :] = dot_t(big, activity_ref[...]) + dot_t(small, activity_ref[...])
        local_ref[rows, :] = value + dot(left_ref[rows, :], right_ref[...])

    for kind, (_, _, third) in enumerate(AXES):
        arrived(gathered[kind].at[pl.ds(0, 48)], recv_2.at[kind])
        for j, offset in enumerate(OFFSETS):
            first = (kind * 3 + j) * SLOTS
            for slot in range(SLOTS):
                staged[first + slot] = gathered[kind][index_ref[kind * 5 + j, slot]]
            remote(
                staged.at[pl.ds(first, SLOTS)], landed[kind].at[pl.ds(here[third] * SLOTS, SLOTS)],
                send_sem.at[3], recv_3.at[kind], device_of(moved(here, third, offset)),
            ).start()
        for slot in range(SLOTS):
            landed[kind][here[third] * SLOTS + slot] = gathered[kind][index_ref[kind * 5 + 3, slot]]

    for kind in range(3):
        arrived(landed[kind].at[pl.ds(0, 36)], recv_3.at[kind])
        first = kind * 24 + core * SLOTS
        for slot in range(SLOTS):
            far_ref[first + slot] = landed[kind][index_ref[kind * 5 + 4, slot]]
        part = far_ref.at[pl.ds(first, SLOTS)]
        remote(part, part, send_sem.at[4], recv_4, device_of(sibling)).start()

    arrived(far_ref.at[pl.ds(0, 36)], recv_4)
    for i, ref in enumerate(
        (
            gathered_0.at[pl.ds(0, 42)], near_ref.at[pl.ds(0, 36)], w_long_ref.at[pl.ds(0, 48)],
            staged, far_ref.at[pl.ds(0, 36)],
        )
    ):
        arrived(ref, send_sem.at[i])


def synapse_kernel(
    far_ref, local_ref, w_long_ref, high_ref, low_ref, left_ref, current_near, cross_near, alive_ref,
    spikes_ref, release_ref, potential_ref, pre_ref, post_ref,
    voltage_ref, volley_ref, presyn_ref, postsyn_ref, local_hbm, long_hbm,
    long_out, right_ref, activity_ref, current_ref, out_sem,
):
    local_copy = pltpu.make_async_copy(local_ref, local_hbm, out_sem.at[OWN // ROWS])
    local_copy.start()
    act_1, pre_1, act_2 = (
        jnp.concatenate([far_ref[kind * 24 + h * SLOTS + s] for s in range(SLOTS) for h in range(2)], axis=1)
        for kind in range(3)
    )
    right_ref[...] = right_matrix(act_1, pre_1, act_2)
    activity_ref[...] = activity_matrix(act_1, act_2)

    def long_copy(step):
        rows = row_block(step)
        return pltpu.make_async_copy(long_out.at[rows], long_hbm.at[rows], out_sem.at[step])

    @pl.loop(0, OWN // ROWS)
    def _(step):
        rows = row_block(step)
        long_out[rows, :] = w_long_ref[rows, :] + dot(left_ref[rows, :], right_ref[...])
        long_copy(step).start()

    @pl.loop(0, OWN // ROWS)
    def _(step):
        rows = row_block(step)
        current_ref[rows, :] = (
            current_near[rows, :]
            + dot_t(high_ref[rows, :], activity_ref[...]) + dot_t(low_ref[rows, :], activity_ref[...])
        )

    alive = alive_ref[...]
    firing_1, activity_1, presyn_1, volley_1, firing_2, activity_2 = early_dynamics(
        spikes_ref[...], release_ref[...], pre_ref[...], alive
    )
    post_1 = post_ref[...]
    post_2 = (postsyn_trace_decay * post_1 + firing_1) * alive
    presyn_ref[...] = (pre_decay * presyn_1 + activity_2) * alive
    postsyn_ref[...] = (postsyn_trace_decay * post_2 + firing_2) * alive
    volley_ref[...] = volley_1 + recovery * (1.0 - volley_1) - depletion * activity_2

    cross = cross_near[...] + cross_products(act_1, pre_1, activity_ref[...])
    cross = adaptation_speed * (cross[:, 8:16] + cross[:, 24:32])
    current = current_ref[...].T
    current_1 = current[0:8] + current[16:24]
    current_2 = current[8:16] + current[24:32]
    extra = lax.dot_general(
        cross, jnp.concatenate([firing_1, -post_1], axis=0), (((0,), (0,)), ((), ())),
        preferred_element_type=jnp.float32, precision=lax.Precision.HIGHEST,
    )
    voltage_1 = (leak_factor * potential_ref[...] + current_1) * alive
    voltage_ref[...] = (leak_factor * voltage_1 + (current_2 + extra)) * alive

    @pl.loop(0, OWN // ROWS)
    def _(step):
        long_copy(step).wait()
    local_copy.wait()


def local(spikes, release, potential, pre_trace, post_trace, w_local, w_long, sources, counts):
    hbm = pl.BlockSpec(memory_space=pltpu.HBM)
    vmem = pl.BlockSpec(memory_space=pltpu.VMEM)
    dma = pltpu.SemaphoreType.DMA
    f32, bf16 = jnp.float32, jnp.bfloat16
    in_hbm = functools.partial(pltpu.with_memory_space_constraint, memory_space=pltpu.HBM)
    parts = pl.pallas_call(
        exchange_kernel,
        name="exchange",
        out_shape=(
            pltpu.VMEM((72, *TILE), f32),
            pltpu.VMEM((OWN, AREA), f32),
            pltpu.VMEM((OWN, FAR), f32),
            pltpu.VMEM((OWN, FAR), bf16),
            pltpu.VMEM((OWN, FAR), bf16),
            pltpu.VMEM((OWN, 80), bf16),
            pltpu.VMEM((OWN, 32), f32),
            pltpu.VMEM((16, 32), f32),
            pltpu.VMEM((TRIALS, OWN), f32),
        ),
        in_specs=[hbm] * 8,
        out_specs=(vmem,) * 9,
        scratch_shapes=[
            pltpu.SMEM((SLOTS, 32), jnp.int32),
            pltpu.SMEM((32,), jnp.int32),
            pltpu.SMEM((15, SLOTS), jnp.int32),
            pltpu.VMEM((2, TRIALS, OWN), jnp.int32),
            *[pltpu.VMEM((TRIALS, OWN), f32)] * 3,
            pltpu.VMEM((48, *TILE), f32),
            *[pltpu.VMEM((64, *TILE), f32)] * 3,
            pltpu.VMEM((108, *TILE), f32),
            *[pltpu.VMEM((48, *TILE), f32)] * 3,
            pltpu.VMEM((80, AREA), bf16),
            pltpu.VMEM((32, AREA), bf16),
            dma((5,)), dma, dma((2,)), dma((3,)), dma((3, 4)), dma((3,)), dma((3,)), dma, dma((5,)),
        ],
        compiler_params=pltpu.CompilerParams(
            collective_id=0, has_side_effects=True, vmem_limit_bytes=28 << 20
        ),
    )(
        in_hbm(sources.T), in_hbm(counts),
        *(in_hbm(x) for x in (spikes, release, pre_trace, post_trace, w_local, w_long)),
    )
    return pl.pallas_call(
        synapse_kernel,
        name="synapses",
        out_shape=(
            *(jax.ShapeDtypeStruct((TRIALS, OWN), f32) for _ in range(4)),
            jax.ShapeDtypeStruct((OWN, AREA), f32),
            jax.ShapeDtypeStruct((OWN, FAR), f32),
        ),
        in_specs=[vmem] * 14,
        out_specs=(vmem, vmem, vmem, vmem, hbm, hbm),
        scratch_shapes=[
            pltpu.VMEM((OWN, FAR), f32),
            pltpu.VMEM((80, FAR), bf16),
            pltpu.VMEM((32, FAR), bf16),
            pltpu.VMEM((OWN, 32), f32),
            dma((OWN // ROWS + 1,)),
        ],
        compiler_params=pltpu.CompilerParams(vmem_limit_bytes=34 << 20),
    )(*parts, spikes, release, potential, pre_trace, post_trace)


def solution(mesh):
    neurons = P(None, ("area", "inarea"))
    synapses = P(("area", "inarea"), None)
    return jax.shard_map(
        local,
        mesh=mesh,
        in_specs=(
            P(None, None, ("area", "inarea")), neurons, neurons, neurons, neurons,
            synapses, synapses, P(), P(),
        ),
        out_specs=(neurons, neurons, neurons, neurons, synapses, synapses),
        check_vma=False,
    )
```
